32 devices in a mesh: tm: 2 (over core), space: 16 (over z, y, x).
Axes of the slice: x: 2, y: 2, z: 4, core: 2. Of those that a mesh axis runs over, the one named last changes fastest.
Arguments:
- fine: bfloat16 [8, 64, 256, 256], P('tm', 'space'), may hold values from -6 to 6
- coarse: bfloat16 [8, 32, 128, 256], P('tm', 'space'), may hold values from -6 to 6
- w_query: bfloat16 [256, 256], replicated, may hold values from -24 to 24
- w_key: bfloat16 [256, 256], replicated, may hold values from -0.375 to 0.375
- w_value: bfloat16 [256, 256], replicated, may hold values from -0.375 to 0.375
- w_out: bfloat16 [256, 256], replicated, may hold values from -0.375 to 0.375
- conv_first: bfloat16 [3, 3, 256, 256], replicated, may hold values from -0.125 to 0.125
- conv_second: bfloat16 [3, 3, 256, 256], replicated, may hold values from -0.125 to 0.125
Outputs:
- joined: bfloat16 [8, 64, 256, 256], P('tm', 'space')
The draws below stay inside these ranges and needn't reach their ends.
All inputs are finite; a program needn't handle non-finite values.
Results may differ from the reference program's by a relative error of at most 0.009.
Values may be sent and summed in bfloat16 or wider, within the bound.
A program may use at most 128 MiB of HBM per device.

```python
import jax
import jax.numpy as jnp
from jax import lax

C = 256
HEADS = 8
W = 256
FRAMES = 8
H = 64


def draw_w_query(key, part):
    base = jax.random.normal(jax.random.fold_in(key, 11), (C, C), jnp.float32) / jnp.sqrt(jnp.float32(C))
    base = jnp.clip(base, -6.0 / jnp.sqrt(jnp.float32(C)), 6.0 / jnp.sqrt(jnp.float32(C)))
    logs = jax.random.uniform(jax.random.fold_in(key, 12), (HEADS,), jnp.float32, jnp.log(0.5), jnp.log(3.0))
    columns = jnp.repeat(jnp.exp(logs), C // HEADS)
    return (base * columns[None, :]).astype(jnp.bfloat16)


def shard_levels(own_key, extent, split, least, high):
    loudness, own = 1.0, jax.random.fold_in(own_key, 6)
    for axis_at, blocks in split:
        heights = jnp.exp(jax.random.uniform(jax.random.fold_in(own, axis_at), (blocks,), jnp.float32, least / len(split), high / len(split)))
        loudness = loudness * jnp.repeat(heights, extent[axis_at] // blocks).reshape([-1 if axis == axis_at else 1 for axis in range(len(extent))])
    return loudness


def scatter_about(own_key, extent, deviation, reach, shards=(), kind=jnp.bfloat16):
    entries = jax.random.normal(own_key, extent, jnp.float32) * deviation
    if len(shards) > 0:
        entries = shard_levels(own_key, extent, shards, -0.22, 0.18) * entries
    return jnp.clip(entries, min=-reach, max=reach).astype(kind)


def setup_inputs(seed: int = 0) -> dict:
    arg_keys = jax.random.split(jax.random.key(seed), 9)
    return {
        "fine": scatter_about(arg_keys[0], (FRAMES, H, W, C), 1.0, 6.0, ((0, 2), (1, 16))),
        "coarse": scatter_about(arg_keys[1], (FRAMES, H // 2, W // 2, C), 1.0, 6.0, ((0, 2), (1, 16))),
        "w_query": draw_w_query(jax.random.fold_in(arg_keys[8], 71), 0),
        "w_key": scatter_about(arg_keys[3], (C, C), C ** -0.5, 0.375),
        "w_value": scatter_about(arg_keys[4], (C, C), C ** -0.5, 0.375),
        "w_out": scatter_about(arg_keys[5], (C, C), C ** -0.5, 0.375),
        "conv_first": scatter_about(arg_keys[6], (3, 3, C, C), (9 * C) ** -0.5, 0.125),
        "conv_second": scatter_about(arg_keys[7], (3, 3, C, C), (9 * C) ** -0.5, 0.125),
    }


def encode(frame_ids, width):
    half = width // 2
    index = jnp.arange(half, dtype=jnp.float32)
    inverse = jnp.exp(-jnp.log(10000.0) * 2.0 * index / width)
    angles = frame_ids.astype(jnp.float32)[:, None] * inverse[None, :]
    return jnp.concatenate([jnp.sin(angles), jnp.cos(angles)], axis=1)

def normalize(features, frame_ids):
    width = features.shape[-1]
    hidden = features.astype(jnp.float32) + encode(frame_ids, width)[:, None, None, :]
    center = hidden - lax.optimization_barrier(jnp.mean(hidden, axis=-1, keepdims=True))
    spread = lax.optimization_barrier(jnp.mean(center * center, axis=-1, keepdims=True))
    return (center * lax.rsqrt(spread + 1e-05)).astype(jnp.bfloat16)

def project(normed, weight):
    shape = normed.shape
    flat = normed.reshape(-1, shape[-1])
    return jnp.dot(flat, weight, preferred_element_type=jnp.float32).astype(jnp.bfloat16).reshape(shape)

def attend(query, key, value):
    frames, rows, cols, width = query.shape
    depth = width // HEADS
    query_heads = query.reshape(frames, rows * cols, HEADS, depth).astype(jnp.float32)
    key_heads = key.reshape(key.shape[0], rows * cols, HEADS, depth).astype(jnp.float32)
    value_heads = value.reshape(value.shape[0], rows * cols, HEADS, depth).astype(jnp.float32)
    scores = jnp.einsum('qphd,kphd->qkhp', query_heads, key_heads) / jnp.sqrt(jnp.float32(depth))
    weights = jax.nn.softmax(scores, axis=1).astype(jnp.bfloat16)
    attended = jnp.einsum('qkhp,kphd->qphd', weights.astype(jnp.float32), value_heads)
    return attended.astype(jnp.bfloat16).reshape(frames, rows, cols, width)

def convolve(features, weight):
    return lax.conv_general_dilated(features.astype(jnp.float32), weight.astype(jnp.float32), (1, 1), 'SAME', dimension_numbers=('NHWC', 'HWIO', 'NHWC'), precision=lax.Precision.HIGHEST)

def double(extended, axis):
    count = extended.shape[axis] - 2
    middle = lax.slice_in_dim(extended, 1, count + 1, axis=axis)
    before = lax.slice_in_dim(extended, 0, count, axis=axis)
    after = lax.slice_in_dim(extended, 2, count + 2, axis=axis)
    even = 0.75 * middle + 0.25 * before
    odd = 0.75 * middle + 0.25 * after
    stacked = jnp.stack([even, odd], axis=axis + 1)
    shape = list(middle.shape)
    shape[axis] = 2 * count
    return stacked.reshape(shape)

def upsample(coarse):
    values = coarse.astype(jnp.float32)
    extended = jnp.pad(values, ((0, 0), (1, 1), (0, 0), (0, 0)), mode='edge')
    rows_done = double(extended, 1)
    extended = jnp.pad(rows_done, ((0, 0), (0, 0), (1, 1), (0, 0)), mode='edge')
    return double(extended, 2)

def reference(fine, coarse, w_query, w_key, w_value, w_out, conv_first, conv_second):
    frame_ids = jnp.arange(fine.shape[0], dtype=jnp.int32)
    normed = normalize(fine, frame_ids)
    query = project(normed, w_query)
    key = project(normed, w_key)
    value = project(normed, w_value)
    attended = attend(query, key, value)
    shape = fine.shape
    branch = jnp.dot(attended.reshape(-1, shape[-1]), w_out, preferred_element_type=jnp.float32).reshape(shape)
    moved = (fine.astype(jnp.float32) + branch).astype(jnp.bfloat16)
    first = convolve(jax.nn.relu(moved), conv_first).astype(jnp.bfloat16)
    second = convolve(jax.nn.relu(first), conv_second)
    up = upsample(coarse)
    return (up + moved.astype(jnp.float32) + second).astype(jnp.bfloat16)
```

```python
import functools

import jax
import jax.numpy as jnp
from jax import lax
from jax.experimental import pallas as pl
from jax.experimental.pallas import tpu as pltpu
from jax.sharding import PartitionSpec as P

HEADS = 8
CHUNKS = 4
TILE = 64
LOG2E = 1.4426950408889634


def encode(frame_ids, width):
    half = width // 2
    index = jnp.arange(half, dtype=jnp.float32)
    inverse = jnp.exp(-jnp.log(10000.0) * 2.0 * index / width)
    angles = frame_ids.astype(jnp.float32)[:, None] * inverse[None, :]
    return jnp.concatenate([jnp.sin(angles), jnp.cos(angles)], axis=1)


def motion_kernel(mine_ref, other_ref, pos_ref, wq_ref, wkv_ref, wo_ref, out_ref):
    own, _, tile, width = mine_ref.shape
    others = other_ref.shape[0]
    depth = width // HEADS
    scale = LOG2E / (float(depth) ** 0.5)
    normed = []
    for frame in range(own + others):
        if frame < own:
            x = mine_ref[frame, 0]
        else:
            x = other_ref[frame - own, 0]
        hidden = x.astype(jnp.float32) + pos_ref[frame : frame + 1, :]
        center = hidden - jnp.mean(hidden, axis=-1, keepdims=True)
        spread = jnp.mean(center * center, axis=-1, keepdims=True)
        normed.append((center * lax.rsqrt(spread + 1e-05)).astype(jnp.bfloat16))
    flat = jnp.concatenate(normed, axis=0)
    query = jnp.dot(flat[: own * tile], wq_ref[...], preferred_element_type=jnp.float32)
    query = query.astype(jnp.bfloat16).reshape(own, tile, width)
    both = jnp.dot(flat, wkv_ref[...], preferred_element_type=jnp.float32).astype(jnp.bfloat16)
    key, value = both[:, :width], both[:, width:]
    rows = lax.broadcasted_iota(jnp.int32, (width, width), 0) // depth
    cols = lax.broadcasted_iota(jnp.int32, (width, width), 1) // depth
    blocks = jnp.where(rows == cols, 1.0, 0.0).astype(jnp.bfloat16)
    scores = []
    for other in range(own + others):
        product = query * key[other * tile : (other + 1) * tile][None]
        scores.append(jnp.dot(product.reshape(own * tile, width), blocks, preferred_element_type=jnp.float32))
    largest = functools.reduce(jnp.maximum, scores)
    total, summed = None, None
    for other, score in enumerate(scores):
        power = jnp.exp2((score - largest) * scale).reshape(own, tile, width)
        term = power * value[other * tile : (other + 1) * tile].astype(jnp.float32)[None]
        total = power if total is None else total + power
        summed = term if summed is None else summed + term
    attended = (summed / total).astype(jnp.bfloat16).reshape(own * tile, width)
    branch = jnp.dot(attended, wo_ref[...], preferred_element_type=jnp.float32)
    branch = branch.reshape(own, tile, width)
    out_ref[0, :, 0] = (mine_ref[:, 0].astype(jnp.float32) + branch).astype(jnp.bfloat16)


def motion(fine, other, chunk, pos, wq, wkv, wo):
    own, rows, cols, width = fine.shape
    others, _, span, _ = other.shape
    tile = min(TILE, span)
    steps = span // tile
    half = rows // 2
    return pl.pallas_call(
        motion_kernel,
        grid=(rows, steps),
        in_specs=[
            pl.BlockSpec((own, 1, tile, width), lambda r, j: (0, r, chunk * steps + j, 0)),
            pl.BlockSpec((others, 1, tile, width), lambda r, j: (0, r, j, 0)),
            pl.BlockSpec(pos.shape, lambda r, j: (0, 0)),
            pl.BlockSpec(wq.shape, lambda r, j: (0, 0)),
            pl.BlockSpec(wkv.shape, lambda r, j: (0, 0)),
            pl.BlockSpec(wo.shape, lambda r, j: (0, 0)),
        ],
        out_specs=pl.BlockSpec((1, own, 1, tile, width), lambda r, j: (r // half, 0, r % half, j, 0)),
        out_shape=jax.ShapeDtypeStruct((2, own, half, span, width), jnp.bfloat16),
        compiler_params=pltpu.CompilerParams(vmem_limit_bytes=48 * 1024 * 1024),
        cost_estimate=pl.CostEstimate(flops=own * rows * span * width * width * 30, bytes_accessed=fine.size * 6 // CHUNKS, transcendentals=own * rows * span * width * 8),
        name="motion",
    )(fine, other, pos, wq, wkv, wo)


def spread_columns(ref, at, row, cols):
    column = lax.broadcasted_iota(jnp.int32, row.shape, 0)
    left = jnp.where(column == 0, 0.0, pltpu.roll(row, 1, 0))
    right = jnp.where(column == cols - 1, 0.0, pltpu.roll(row, cols - 1, 0))
    width = row.shape[1]
    ref[at * cols : (at + 1) * cols, :width] = left.astype(jnp.bfloat16)
    ref[at * cols : (at + 1) * cols, width : 2 * width] = row.astype(jnp.bfloat16)
    ref[at * cols : (at + 1) * cols, 2 * width :] = right.astype(jnp.bfloat16)


def conv_rows(ref, start, count, cols, weight_ref):
    pieces = [ref[(start + step) * cols : (start + step + count) * cols, :] for step in range(3)]
    return jnp.dot(jnp.concatenate(pieces, axis=1), weight_ref[...], preferred_element_type=jnp.float32)


def conv_kernel(chunks, flags_ref, *refs):
    moved_refs = refs[:chunks]
    before_refs = refs[chunks : 2 * chunks]
    after_refs = refs[2 * chunks : 3 * chunks]
    coarse_ref, above_ref, below_ref, lift_ref, w1_ref, w2_ref, out_ref, x_ref, f_ref = refs[3 * chunks :]
    _, rows, cols, width = out_ref.shape
    half = rows // 2
    is_first = flags_ref[0] == 1
    is_last = flags_ref[1] == 1

    def line(r):
        if r < 0:
            parts = [ref[0, r + 2] for ref in before_refs]
        elif r < rows:
            parts = [ref[r // half, 0, r % half] for ref in moved_refs]
        else:
            parts = [ref[0, r - rows] for ref in after_refs]
        return jnp.concatenate(parts, axis=0).astype(jnp.float32)

    for r in range(-2, rows + 2):
        spread_columns(x_ref, r + 2, jnp.maximum(line(r), 0.0), cols)
    for r in range(-1, rows + 1):
        first = conv_rows(x_ref, r + 1, 1, cols, w1_ref)
        first = jnp.maximum(first, 0.0).astype(jnp.bfloat16).astype(jnp.float32)
        if r == -1:
            first = jnp.where(is_first, 0.0, first)
        if r == rows:
            first = jnp.where(is_last, 0.0, first)
        spread_columns(f_ref, r + 1, first, cols)
    top = jnp.where(is_first, coarse_ref[0, 0], above_ref[0, 0])
    bottom = jnp.where(is_last, coarse_ref[0, half - 1], below_ref[0, 0])
    coarse = [top] + [coarse_ref[0, i] for i in range(half)] + [bottom]
    for r in range(rows):
        near = coarse[r // 2 + 1]
        far = coarse[r // 2] if r % 2 == 0 else coarse[r // 2 + 2]
        up = jnp.dot(lift_ref[...], jnp.concatenate([near, far], axis=0), preferred_element_type=jnp.float32)
        second = conv_rows(f_ref, r, 1, cols, w2_ref)
        out_ref[0, r] = (up + line(r) + second).astype(jnp.bfloat16)


def convolutions(flags, moved, before, after, coarse, above, below, lift, w1, w2, rows):
    _, own, half, span, width = moved[0].shape
    chunks = len(moved)
    cols = span * chunks
    small = coarse.shape[2]
    in_specs = [pl.BlockSpec(memory_space=pltpu.SMEM)]
    in_specs += [pl.BlockSpec((2, 1, half, span, width), lambda f: (0, f, 0, 0, 0))] * chunks
    in_specs += [pl.BlockSpec((1, 2, span, width), lambda f: (f, 0, 0, 0))] * (2 * chunks)
    in_specs += [pl.BlockSpec((1, half, small, width), lambda f: (f, 0, 0, 0))]
    in_specs += [pl.BlockSpec((1, 1, small, width), lambda f: (f, 0, 0, 0))] * 2
    in_specs += [pl.BlockSpec(a.shape, lambda f: (0, 0)) for a in (lift, w1, w2)]
    return pl.pallas_call(
        functools.partial(conv_kernel, chunks),
        grid=(own,),
        in_specs=in_specs,
        out_specs=pl.BlockSpec((1, rows, cols, width), lambda f: (f, 0, 0, 0)),
        out_shape=jax.ShapeDtypeStruct((own, rows, cols, width), jnp.bfloat16),
        scratch_shapes=[
            pltpu.VMEM(((rows + 4) * cols, 3 * width), jnp.bfloat16),
            pltpu.VMEM(((rows + 2) * cols, 3 * width), jnp.bfloat16),
        ],
        compiler_params=pltpu.CompilerParams(vmem_limit_bytes=56 * 1024 * 1024),
        cost_estimate=pl.CostEstimate(flops=own * rows * cols * width * width * 45, bytes_accessed=own * rows * cols * width * 8, transcendentals=0),
        name="convolutions",
    )(flags, *moved, *before, *after, coarse, above, below, lift, w1, w2)


def lift_matrix(small):
    out = jnp.arange(2 * small)[:, None]
    source = jnp.arange(small)[None, :]
    near = out // 2
    far = jnp.clip(jnp.where(out % 2 == 0, near - 1, near + 1), 0, small - 1)
    base = 0.75 * (source == near) + 0.25 * (source == far)
    return jnp.concatenate([0.75 * base, 0.25 * base], axis=1).astype(jnp.bfloat16)


def local(fine, coarse, w_query, w_key, w_value, w_out, conv_first, conv_second):
    own, rows, cols, width = fine.shape
    bands, halves = lax.axis_size("space"), lax.axis_size("tm")
    place, mine = lax.axis_index("space"), lax.axis_index("tm")
    up = [(i, i + 1) for i in range(bands - 1)]
    down = [(i + 1, i) for i in range(bands - 1)]
    above = lax.ppermute(coarse[:, -1:], "space", up)
    below = lax.ppermute(coarse[:, :1], "space", down)
    frames = jnp.arange(own, dtype=jnp.int32)
    ids = [lax.rem(mine + shift, halves) * own + frames for shift in range(halves)]
    pos = encode(jnp.concatenate(ids), width)
    wkv = jnp.concatenate([w_key, w_value], axis=1)
    w1 = conv_first.reshape(9 * width, width)
    w2 = conv_second.reshape(9 * width, width)
    flags = jnp.stack([place == 0, place == bands - 1]).astype(jnp.int32)
    span = cols // CHUNKS
    moved, before, after = [], [], []
    for chunk in range(CHUNKS):
        piece = fine[:, :, chunk * span : (chunk + 1) * span]
        rest = []
        for shift in range(1, halves):
            rest.append(lax.ppermute(piece, "tm", [((i + shift) % halves, i) for i in range(halves)]))
        other = rest[0] if len(rest) == 1 else jnp.concatenate(rest, axis=0)
        block = motion(fine, other, chunk, pos, w_query, wkv, w_out)
        moved.append(block)
        before.append(lax.ppermute(block[1][:, -2:], "space", up))
        after.append(lax.ppermute(block[0][:, :2], "space", down))
    return convolutions(flags, moved, before, after, coarse, above, below, lift_matrix(coarse.shape[2]), w1, w2, rows)


def solution(mesh):
    return jax.shard_map(
        local,
        mesh=mesh,
        in_specs=(
            P("tm", "space", None, None),
            P("tm", "space", None, None),
            P(),
            P(),
            P(),
            P(),
            P(),
            P(),
        ),
        out_specs=P("tm", "space", None, None),
        check_vma=False,
    )
```

```python
import functools

import jax
import jax.numpy as jnp
import numpy as np
from jax import lax
from jax.experimental import pallas as pl
from jax.experimental.pallas import tpu as pltpu
from jax.sharding import PartitionSpec as P

HEADS = 8
CHUNKS = 4
HALO = 2
LOG2E = 1.4426950408889634
MESH = pl.DeviceIdType.MESH


def encode(frames, width):
    half = width // 2
    inverse = np.exp(-np.log(10000.0) * 2.0 * np.arange(half) / width)
    angles = np.arange(frames)[:, None] * inverse[None, :]
    return np.concatenate([np.sin(angles), np.cos(angles)], axis=1).astype(np.float32)


def lift_matrix(small):
    out = np.arange(2 * small)[:, None]
    source = np.arange(small)[None, :]
    near = out // 2
    far = np.clip(np.where(out % 2 == 0, near - 1, near + 1), 0, small - 1)
    base = 0.75 * (source == near) + 0.25 * (source == far)
    return np.concatenate([0.75 * base, 0.25 * base], axis=1).astype(jnp.bfloat16)


def attention(mine, others, pos, wq_ref, wk_ref, wv_ref, wo_ref):
    own, (tile, width) = len(mine), mine[0].shape
    depth = width // HEADS
    scale = LOG2E / (float(depth) ** 0.5)
    normed = []
    for x, place in zip(mine + others, pos):
        hidden = x.astype(jnp.float32) + place
        center = hidden - jnp.mean(hidden, axis=-1, keepdims=True)
        spread = jnp.mean(center * center, axis=-1, keepdims=True)
        normed.append((center * lax.rsqrt(spread + 1e-05)).astype(jnp.bfloat16))
    flat = jnp.concatenate(normed, axis=0)
    query = jnp.dot(flat[: own * tile], wq_ref[...], preferred_element_type=jnp.float32)
    query = query.astype(jnp.bfloat16).reshape(own, tile, width)
    key = jnp.dot(flat, wk_ref[...], preferred_element_type=jnp.float32).astype(jnp.bfloat16)
    value = jnp.dot(flat, wv_ref[...], preferred_element_type=jnp.float32).astype(jnp.bfloat16)
    rows = lax.broadcasted_iota(jnp.int32, (width, width), 0) // depth
    cols = lax.broadcasted_iota(jnp.int32, (width, width), 1) // depth
    blocks = jnp.where(rows == cols, 1.0, 0.0).astype(jnp.bfloat16)
    scores = []
    for at in range(len(normed)):
        product = query * key[at * tile : (at + 1) * tile][None]
        scores.append(jnp.dot(product.reshape(own * tile, width), blocks, preferred_element_type=jnp.float32))
    largest = functools.reduce(jnp.maximum, scores)
    total, summed = None, None
    for at, score in enumerate(scores):
        power = jnp.exp2((score - largest) * scale).reshape(own, tile, width)
        term = power * value[at * tile : (at + 1) * tile].astype(jnp.float32)[None]
        total = power if total is None else total + power
        summed = term if summed is None else summed + term
    attended = (summed / total).astype(jnp.bfloat16).reshape(own * tile, width)
    branch = jnp.dot(attended, wo_ref[...], preferred_element_type=jnp.float32)
    return branch.reshape(own, tile, width)


def spread_columns(ref, at, row, cols):
    column = lax.broadcasted_iota(jnp.int32, row.shape, 0)
    left = jnp.where(column == 0, 0.0, pltpu.roll(row, 1, 0))
    right = jnp.where(column == cols - 1, 0.0, pltpu.roll(row, cols - 1, 0))
    width = row.shape[1]
    ref[at * cols : (at + 1) * cols, :width] = left.astype(jnp.bfloat16)
    ref[at * cols : (at + 1) * cols, width : 2 * width] = row.astype(jnp.bfloat16)
    ref[at * cols : (at + 1) * cols, 2 * width :] = right.astype(jnp.bfloat16)


def conv_rows(ref, start, count, cols, weight_ref):
    pieces = [ref[(start + step) * cols : (start + step + count) * cols, :] for step in range(3)]
    return jnp.dot(jnp.concatenate(pieces, axis=1), weight_ref[...], preferred_element_type=jnp.float32)


def kernel(
    bands, halves, fine_ref, coarse_ref, pos_ref, wq_ref, wk_ref, wv_ref, wo_ref, w1_hbm, w2_hbm, lift_ref, out_ref,
    mine, other, moved, coarse, x_ref, f_ref, w1_ref, w2_ref, outs,
    local_sems, fine_send, fine_recv, halo_send, halo_recv, coarse_send, coarse_recv, out_sems,
):
    own, rows, cols, width = mine.shape
    half = rows // 2
    span = cols // CHUNKS
    early = own // 2
    place, core = lax.axis_index("space"), lax.axis_index("tm")
    has_before, has_after = place > 0, place < bands - 1

    def fine_copy(shift, chunk):
        span_at = pl.ds(pl.multiple_of(chunk * span, span), span)
        return pltpu.make_async_remote_copy(
            src_ref=fine_ref.at[:, :, span_at],
            dst_ref=other.at[pl.ds((shift - 1) * own, own), :, span_at],
            send_sem=fine_send.at[shift - 1, chunk],
            recv_sem=fine_recv.at[shift - 1, chunk],
            device_id={"tm": lax.rem(core + halves - shift, halves)},
            device_id_type=MESH,
        )

    def mine_copy(chunk):
        span_at = pl.ds(pl.multiple_of(chunk * span, span), span)
        return pltpu.make_async_copy(fine_ref.at[:, :, span_at], mine.at[:, :, span_at], local_sems.at[chunk])

    def to_after(src, dst, send, recv):
        return pltpu.make_async_remote_copy(
            src_ref=src, dst_ref=dst, send_sem=send, recv_sem=recv, device_id={"space": place + 1}, device_id_type=MESH
        )

    def to_before(src, dst, send, recv):
        return pltpu.make_async_remote_copy(
            src_ref=src, dst_ref=dst, send_sem=send, recv_sem=recv, device_id={"space": place - 1}, device_id_type=MESH
        )

    def coarse_up():
        return to_after(coarse_ref.at[:, half - 1 : half], coarse.at[:, 0:1], coarse_send.at[0], coarse_recv.at[0])

    def coarse_down():
        return to_before(coarse_ref.at[:, 0:1], coarse.at[:, half + 1 : half + 2], coarse_send.at[1], coarse_recv.at[1])

    def halo_up(frames, span_at, piece):
        return to_after(
            moved.at[frames, rows : rows + HALO, span_at], moved.at[frames, 0:HALO, span_at],
            halo_send.at[0, piece], halo_recv.at[0, piece],
        )

    def halo_down(frames, span_at, piece):
        return to_before(
            moved.at[frames, HALO : 2 * HALO, span_at], moved.at[frames, rows + HALO : rows + 2 * HALO, span_at],
            halo_send.at[1, piece], halo_recv.at[1, piece],
        )

    def both(frames, span_at, piece, act_up, act_down):
        pl.when(has_after)(lambda: act_up(halo_up(frames, span_at, piece)))
        pl.when(has_before)(lambda: act_down(halo_down(frames, span_at, piece)))

    def start(copy):
        copy.start()

    def wait_send(copy):
        copy.wait_send()

    def wait_recv(copy):
        copy.wait_recv()

    def landed(frames, span_at, piece):
        pl.when(has_before)(lambda: halo_up(frames, span_at, piece).wait_recv())
        pl.when(has_after)(lambda: halo_down(frames, span_at, piece).wait_recv())

    for chunk in range(CHUNKS):
        mine_copy(chunk).start()
    own_coarse = pltpu.make_async_copy(coarse_ref, coarse.at[:, 1 : half + 1], local_sems.at[CHUNKS])
    first_weights = pltpu.make_async_copy(w1_hbm, w1_ref, local_sems.at[CHUNKS + 1])
    second_weights = pltpu.make_async_copy(w2_hbm, w2_ref, local_sems.at[CHUNKS + 2])

    barrier = pltpu.get_barrier_semaphore()
    for shift in range(1, halves):
        pl.semaphore_signal(barrier, inc=1, device_id={"tm": lax.rem(core + shift, halves)}, device_id_type=MESH)

    @pl.when(has_before)
    def _():
        pl.semaphore_signal(barrier, inc=1, device_id={"space": place - 1}, device_id_type=MESH)

    @pl.when(has_after)
    def _():
        pl.semaphore_signal(barrier, inc=1, device_id={"space": place + 1}, device_id_type=MESH)

    peers = halves - 1 + has_before.astype(jnp.int32) + has_after.astype(jnp.int32)
    pl.semaphore_wait(barrier, peers)

    for shift in range(1, halves):
        for chunk in range(CHUNKS):
            fine_copy(shift, chunk).start()
    pl.when(has_after)(lambda: coarse_up().start())
    pl.when(has_before)(lambda: coarse_down().start())
    own_coarse.start()
    first_weights.start()
    second_weights.start()

    @pl.when(jnp.logical_not(has_before))
    def _():
        moved[:, 0:HALO] = jnp.zeros((own, HALO, cols, width), jnp.bfloat16)

    @pl.when(jnp.logical_not(has_after))
    def _():
        moved[:, rows + HALO :] = jnp.zeros((own, HALO, cols, width), jnp.bfloat16)

    pos = []
    for shift in range(halves):
        for frame in range(own):
            pos.append(pos_ref[pl.ds(lax.rem(core + shift, halves) * own + frame, 1), :])

    def motion_step(step, carry):
        chunk, row = step // rows, lax.rem(step, rows)
        span_at = pl.ds(pl.multiple_of(chunk * span, span), span)

        @pl.when(row == 0)
        def _():
            mine_copy(chunk).wait()
            for shift in range(1, halves):
                fine_copy(shift, chunk).wait_recv()

        here = [mine[frame, row, span_at, :] for frame in range(own)]
        there = [other[frame, row, span_at, :] for frame in range(own * (halves - 1))]
        branch = attention(here, there, pos, wq_ref, wk_ref, wv_ref, wo_ref)
        for frame in range(own):
            moved[frame, row + HALO, span_at, :] = (here[frame].astype(jnp.float32) + branch[frame]).astype(jnp.bfloat16)

        @pl.when((row == rows - 1) & (chunk == 0))
        def _():
            both(pl.ds(0, own), pl.ds(0, span), 0, start, start)

        @pl.when((row == rows - 1) & (chunk > 0))
        def _():
            both(pl.ds(0, early), span_at, chunk, start, start)

        return carry

    lax.fori_loop(0, CHUNKS * rows, motion_step, 0)
    rest = pl.ds(span, cols - span)
    for frame in range(early, own):
        both(pl.ds(frame, 1), rest, CHUNKS + frame - early, start, start)

    own_coarse.wait()
    first_weights.wait()
    second_weights.wait()
    pl.when(has_before)(lambda: coarse_up().wait_recv())
    pl.when(has_after)(lambda: coarse_down().wait_recv())

    @pl.when(jnp.logical_not(has_before))
    def _():
        coarse[:, 0] = coarse[:, 1]

    @pl.when(jnp.logical_not(has_after))
    def _():
        coarse[:, half + 1] = coarse[:, half]

    def out_copy(frame):
        slot = lax.rem(frame, 2)
        return pltpu.make_async_copy(outs.at[slot], out_ref.at[frame], out_sems.at[slot])

    def conv_step(frame, carry):
        @pl.when(frame == 0)
        def _():
            landed(pl.ds(0, own), pl.ds(0, span), 0)
            for chunk in range(1, CHUNKS):
                landed(pl.ds(0, early), pl.ds(chunk * span, span), chunk)

        @pl.when(frame >= early)
        def _():
            landed(pl.ds(frame, 1), rest, CHUNKS + frame - early)

        for r in range(rows + 2 * HALO):
            spread_columns(x_ref, r, jnp.maximum(moved[frame, r].astype(jnp.float32), 0.0), cols)
        for r in range(rows + 2):
            first = conv_rows(x_ref, r, 1, cols, w1_ref)
            first = jnp.maximum(first, 0.0).astype(jnp.bfloat16).astype(jnp.float32)
            if r == 0:
                first = jnp.where(has_before, first, 0.0)
            if r == rows + 1:
                first = jnp.where(has_after, first, 0.0)
            spread_columns(f_ref, r, first, cols)

        @pl.when(frame >= 2)
        def _():
            out_copy(frame - 2).wait()

        for r in range(rows):
            near = coarse[frame, r // 2 + 1]
            far = coarse[frame, r // 2] if r % 2 == 0 else coarse[frame, r // 2 + 2]
            up = jnp.dot(lift_ref[...], jnp.concatenate([near, far], axis=0), preferred_element_type=jnp.float32)
            second = conv_rows(f_ref, r, 1, cols, w2_ref)
            outs[lax.rem(frame, 2), r] = (up + moved[frame, r + HALO].astype(jnp.float32) + second).astype(jnp.bfloat16)
        out_copy(frame).start()
        return carry

    lax.fori_loop(0, own, conv_step, 0)
    for frame in range(max(own - 2, 0), own):
        out_copy(frame).wait()
    for shift in range(1, halves):
        for chunk in range(CHUNKS):
            fine_copy(shift, chunk).wait_send()
    pl.when(has_after)(lambda: coarse_up().wait_send())
    pl.when(has_before)(lambda: coarse_down().wait_send())
    both(pl.ds(0, own), pl.ds(0, span), 0, wait_send, wait_send)
    for chunk in range(1, CHUNKS):
        both(pl.ds(0, early), pl.ds(chunk * span, span), chunk, wait_send, wait_send)
    for frame in range(early, own):
        both(pl.ds(frame, 1), rest, CHUNKS + frame - early, wait_send, wait_send)


def local(fine, coarse, w_query, w_key, w_value, w_out, conv_first, conv_second):
    own, rows, cols, width = fine.shape
    _, half, small, _ = coarse.shape
    bands, halves = lax.axis_size("space"), lax.axis_size("tm")
    pieces = CHUNKS + own - own // 2
    far = own * (halves - 1)
    any_space = pl.BlockSpec(memory_space=pl.ANY)
    vmem = pl.BlockSpec(memory_space=pltpu.VMEM)
    bf16 = jnp.bfloat16
    return pl.pallas_call(
        functools.partial(kernel, bands, halves),
        in_specs=[any_space] * 2 + [vmem] * 5 + [any_space] * 2 + [vmem],
        out_specs=any_space,
        out_shape=jax.ShapeDtypeStruct(fine.shape, bf16),
        scratch_shapes=[
            pltpu.VMEM((own, rows, cols, width), bf16),
            pltpu.VMEM((far, rows, cols, width), bf16),
            pltpu.VMEM((own, rows + 2 * HALO, cols, width), bf16),
            pltpu.VMEM((own, half + 2, small, width), bf16),
            pltpu.VMEM(((rows + 4) * cols, 3 * width), bf16),
            pltpu.VMEM(((rows + 2) * cols, 3 * width), bf16),
            pltpu.VMEM((9 * width, width), bf16),
            pltpu.VMEM((9 * width, width), bf16),
            pltpu.VMEM((2, rows, cols, width), bf16),
            pltpu.SemaphoreType.DMA((CHUNKS + 3,)),
            pltpu.SemaphoreType.DMA((halves - 1, CHUNKS)),
            pltpu.SemaphoreType.DMA((halves - 1, CHUNKS)),
            pltpu.SemaphoreType.DMA((2, pieces)),
            pltpu.SemaphoreType.DMA((2, pieces)),
            pltpu.SemaphoreType.DMA((2,)),
            pltpu.SemaphoreType.DMA((2,)),
            pltpu.SemaphoreType.DMA((2,)),
        ],
        compiler_params=pltpu.CompilerParams(
            collective_id=0, has_side_effects=True, vmem_limit_bytes=62 * 1024 * 1024
        ),
        name="fused",
    )(
        fine, coarse, jnp.asarray(encode(own * halves, width)), w_query, w_key, w_value, w_out,
        conv_first.reshape(9 * width, width), conv_second.reshape(9 * width, width), jnp.asarray(lift_matrix(small)),
    )


def solution(mesh):
    return jax.shard_map(
        local,
        mesh=mesh,
        in_specs=(
            P("tm", "space", None, None),
            P("tm", "space", None, None),
            P(),
            P(),
            P(),
            P(),
            P(),
            P(),
        ),
        out_specs=P("tm", "space", None, None),
        check_vma=False,
    )
```

```python
import functools

import jax
import jax.numpy as jnp
import numpy as np
from jax import lax
from jax.experimental import pallas as pl
from jax.experimental.pallas import tpu as pltpu
from jax.sharding import PartitionSpec as P

HEADS = 8
CHUNKS = 4
HALO = 1
LOG2E = 1.4426950408889634
MESH = pl.DeviceIdType.MESH


def encode(frames, width):
    half = width // 2
    inverse = np.exp(-np.log(10000.0) * 2.0 * np.arange(half) / width)
    angles = np.arange(frames)[:, None] * inverse[None, :]
    return np.concatenate([np.sin(angles), np.cos(angles)], axis=1).astype(np.float32)


def lift_matrix(small):
    out = np.arange(2 * small)[:, None]
    source = np.arange(small)[None, :]
    near = out // 2
    far = np.clip(np.where(out % 2 == 0, near - 1, near + 1), 0, small - 1)
    base = 0.75 * (source == near) + 0.25 * (source == far)
    return np.concatenate([0.75 * base, 0.25 * base], axis=1).astype(jnp.bfloat16)


def attention(mine, others, pos, wq_ref, wk_ref, wv_ref, wo_ref):
    own, (tile, width) = len(mine), mine[0].shape
    depth = width // HEADS
    scale = LOG2E / (float(depth) ** 0.5)
    normed = []
    for x, place in zip(mine + others, pos):
        hidden = x.astype(jnp.float32) + place
        center = hidden - jnp.mean(hidden, axis=-1, keepdims=True)
        spread = jnp.mean(center * center, axis=-1, keepdims=True)
        normed.append((center * lax.rsqrt(spread + 1e-05)).astype(jnp.bfloat16))
    flat = jnp.concatenate(normed, axis=0)
    query = jnp.dot(flat[: own * tile], wq_ref[...], preferred_element_type=jnp.float32)
    query = query.astype(jnp.bfloat16).reshape(own, tile, width)
    key = jnp.dot(flat, wk_ref[...], preferred_element_type=jnp.float32).astype(jnp.bfloat16)
    value = jnp.dot(flat, wv_ref[...], preferred_element_type=jnp.float32).astype(jnp.bfloat16)
    rows = lax.broadcasted_iota(jnp.int32, (width, width), 0) // depth
    cols = lax.broadcasted_iota(jnp.int32, (width, width), 1) // depth
    blocks = jnp.where(rows == cols, 1.0, 0.0).astype(jnp.bfloat16)
    scores = []
    for at in range(len(normed)):
        product = query * key[at * tile : (at + 1) * tile][None]
        scores.append(jnp.dot(product.reshape(own * tile, width), blocks, preferred_element_type=jnp.float32))
    largest = functools.reduce(jnp.maximum, scores)
    total, summed = None, None
    for at, score in enumerate(scores):
        power = jnp.exp2((score - largest) * scale).reshape(own, tile, width)
        term = power * value[at * tile : (at + 1) * tile].astype(jnp.float32)[None]
        total = power if total is None else total + power
        summed = term if summed is None else summed + term
    attended = (summed / total).astype(jnp.bfloat16).reshape(own * tile, width)
    branch = jnp.dot(attended, wo_ref[...], preferred_element_type=jnp.float32)
    return branch.reshape(own, tile, width)


def spread_columns(ref, at, row, cols):
    column = lax.broadcasted_iota(jnp.int32, row.shape, 0)
    left = jnp.where(column == 0, 0.0, pltpu.roll(row, 1, 0))
    right = jnp.where(column == cols - 1, 0.0, pltpu.roll(row, cols - 1, 0))
    width = row.shape[1]
    ref[at * cols : (at + 1) * cols, :width] = left.astype(jnp.bfloat16)
    ref[at * cols : (at + 1) * cols, width : 2 * width] = row.astype(jnp.bfloat16)
    ref[at * cols : (at + 1) * cols, 2 * width :] = right.astype(jnp.bfloat16)


def conv_rows(ref, start, first, last, cols, weight_ref):
    pieces = [ref[(start + step) * cols : (start + step + 1) * cols, :] for step in range(first, last)]
    depth = ref.shape[1]
    return jnp.dot(
        jnp.concatenate(pieces, axis=1), weight_ref[first * depth : last * depth, :], preferred_element_type=jnp.float32
    )


def kernel(
    bands, halves, fine_ref, coarse_ref, pos_ref, wq_ref, wk_ref, wv_ref, wo_ref, w1_hbm, w2_hbm, lift_ref, out_ref,
    mine, other, moved, coarse, x_ref, f_ref, w1_ref, w2_ref, edges, part_out, part_in,
    local_sems, fine_send, fine_recv, halo_send, halo_recv, part_send, part_recv, out_sems,
):
    own, rows, cols, width = mine.shape
    half = rows // 2
    span = cols // CHUNKS
    early = own // 2
    place, core = lax.axis_index("space"), lax.axis_index("tm")
    has_before, has_after = place > 0, place < bands - 1

    def fine_copy(shift, chunk):
        span_at = pl.ds(pl.multiple_of(chunk * span, span), span)
        return pltpu.make_async_remote_copy(
            src_ref=fine_ref.at[:, :, span_at],
            dst_ref=other.at[pl.ds((shift - 1) * own, own), :, span_at],
            send_sem=fine_send.at[shift - 1, chunk],
            recv_sem=fine_recv.at[shift - 1, chunk],
            device_id={"tm": lax.rem(core + halves - shift, halves)},
            device_id_type=MESH,
        )

    def mine_copy(chunk):
        span_at = pl.ds(pl.multiple_of(chunk * span, span), span)
        return pltpu.make_async_copy(fine_ref.at[:, :, span_at], mine.at[:, :, span_at], local_sems.at[chunk])

    def to_after(src, dst, send, recv):
        return pltpu.make_async_remote_copy(
            src_ref=src, dst_ref=dst, send_sem=send, recv_sem=recv, device_id={"space": place + 1}, device_id_type=MESH
        )

    def to_before(src, dst, send, recv):
        return pltpu.make_async_remote_copy(
            src_ref=src, dst_ref=dst, send_sem=send, recv_sem=recv, device_id={"space": place - 1}, device_id_type=MESH
        )

    def part_up(frame):
        return to_after(part_out.at[0, frame], part_in.at[0, frame], part_send.at[0, frame], part_recv.at[0, frame])

    def part_down(frame):
        return to_before(part_out.at[1, frame], part_in.at[1, frame], part_send.at[1, frame], part_recv.at[1, frame])

    def halo_up(frames, span_at, piece):
        return to_after(
            moved.at[frames, rows : rows + HALO, span_at], moved.at[frames, 0:HALO, span_at],
            halo_send.at[0, piece], halo_recv.at[0, piece],
        )

    def halo_down(frames, span_at, piece):
        return to_before(
            moved.at[frames, HALO : 2 * HALO, span_at], moved.at[frames, rows + HALO : rows + 2 * HALO, span_at],
            halo_send.at[1, piece], halo_recv.at[1, piece],
        )

    def both(frames, span_at, piece, act_up, act_down):
        pl.when(has_after)(lambda: act_up(halo_up(frames, span_at, piece)))
        pl.when(has_before)(lambda: act_down(halo_down(frames, span_at, piece)))

    def start(copy):
        copy.start()

    def wait_send(copy):
        copy.wait_send()

    def wait_recv(copy):
        copy.wait_recv()

    def landed(frames, span_at, piece):
        pl.when(has_before)(lambda: halo_up(frames, span_at, piece).wait_recv())
        pl.when(has_after)(lambda: halo_down(frames, span_at, piece).wait_recv())

    for chunk in range(CHUNKS):
        mine_copy(chunk).start()
    own_coarse = pltpu.make_async_copy(coarse_ref, coarse, local_sems.at[CHUNKS])
    first_weights = pltpu.make_async_copy(w1_hbm, w1_ref, local_sems.at[CHUNKS + 1])
    second_weights = pltpu.make_async_copy(w2_hbm, w2_ref, local_sems.at[CHUNKS + 2])

    barrier = pltpu.get_barrier_semaphore()
    for shift in range(1, halves):
        pl.semaphore_signal(barrier, inc=1, device_id={"tm": lax.rem(core + shift, halves)}, device_id_type=MESH)

    @pl.when(has_before)
    def _():
        pl.semaphore_signal(barrier, inc=1, device_id={"space": place - 1}, device_id_type=MESH)

    @pl.when(has_after)
    def _():
        pl.semaphore_signal(barrier, inc=1, device_id={"space": place + 1}, device_id_type=MESH)

    peers = halves - 1 + has_before.astype(jnp.int32) + has_after.astype(jnp.int32)
    pl.semaphore_wait(barrier, peers)

    for shift in range(1, halves):
        for chunk in range(CHUNKS):
            fine_copy(shift, chunk).start()
    own_coarse.start()
    first_weights.start()
    second_weights.start()

    @pl.when(jnp.logical_not(has_before))
    def _():
        moved[:, 0:HALO] = jnp.zeros((own, HALO, cols, width), jnp.bfloat16)
        part_in[0] = jnp.zeros((own, cols, width), jnp.bfloat16)

    @pl.when(jnp.logical_not(has_after))
    def _():
        moved[:, rows + HALO :] = jnp.zeros((own, HALO, cols, width), jnp.bfloat16)
        part_in[1] = jnp.zeros((own, cols, width), jnp.bfloat16)

    pos = []
    for shift in range(halves):
        for frame in range(own):
            pos.append(pos_ref[pl.ds(lax.rem(core + shift, halves) * own + frame, 1), :])

    def motion_tile(chunk, row):
        span_at = pl.ds(pl.multiple_of(chunk * span, span), span)
        here = [mine[frame, row, span_at, :] for frame in range(own)]
        there = [other[frame, row, span_at, :] for frame in range(own * (halves - 1))]
        branch = attention(here, there, pos, wq_ref, wk_ref, wv_ref, wo_ref)
        for frame in range(own):
            moved[frame, row + HALO, span_at, :] = (here[frame].astype(jnp.float32) + branch[frame]).astype(jnp.bfloat16)

    def edge_step(step, carry):
        chunk, edge = step // 2, lax.rem(step, 2)
        span_at = pl.ds(pl.multiple_of(chunk * span, span), span)

        @pl.when(edge == 0)
        def _():
            mine_copy(chunk).wait()
            for shift in range(1, halves):
                fine_copy(shift, chunk).wait_recv()

        motion_tile(chunk, edge * (rows - 1))

        @pl.when((edge == 1) & (chunk == 0))
        def _():
            both(pl.ds(0, own), pl.ds(0, span), 0, start, start)

        @pl.when((edge == 1) & (chunk > 0))
        def _():
            both(pl.ds(0, early), span_at, chunk, start, start)

        return carry

    def inner_step(step, carry):
        motion_tile(step // (rows - 2), 1 + lax.rem(step, rows - 2))
        return carry

    lax.fori_loop(0, CHUNKS * 2, edge_step, 0)
    rest = pl.ds(span, cols - span)
    for frame in range(early, own):
        both(pl.ds(frame, 1), rest, CHUNKS + frame - early, start, start)
    lax.fori_loop(0, CHUNKS * (rows - 2), inner_step, 0)

    own_coarse.wait()
    first_weights.wait()
    second_weights.wait()

    def inner_copy(frame):
        return pltpu.make_async_copy(
            mine.at[frame, 1 : rows - 1], out_ref.at[frame, 1 : rows - 1], out_sems.at[0, frame]
        )

    def edge_copy(frame, side):
        row = side * (rows - 1)
        return pltpu.make_async_copy(mine.at[frame, row], out_ref.at[frame, row], out_sems.at[1 + side, frame])

    def lifted(near, far):
        return jnp.dot(lift_ref[...], jnp.concatenate([near, far], axis=0), preferred_element_type=jnp.float32)

    def conv_step(frame, carry):
        @pl.when(frame == 0)
        def _():
            landed(pl.ds(0, own), pl.ds(0, span), 0)
            for chunk in range(1, CHUNKS):
                landed(pl.ds(0, early), pl.ds(chunk * span, span), chunk)

        @pl.when(frame >= early)
        def _():
            landed(pl.ds(frame, 1), rest, CHUNKS + frame - early)

        for r in range(rows + 2 * HALO):
            spread_columns(x_ref, r, jnp.maximum(moved[frame, r].astype(jnp.float32), 0.0), cols)
        for r in range(rows):
            first = conv_rows(x_ref, r, 0, 3, cols, w1_ref)
            first = jnp.maximum(first, 0.0).astype(jnp.bfloat16).astype(jnp.float32)
            spread_columns(f_ref, r, first, cols)
        top, bottom = coarse[frame, 0], coarse[frame, half - 1]
        none = jnp.zeros_like(top)
        part = conv_rows(f_ref, rows - 1, 0, 1, cols, w2_ref) + lifted(none, bottom)
        part_out[0, frame] = part.astype(jnp.bfloat16)
        part = conv_rows(f_ref, -2, 2, 3, cols, w2_ref) + lifted(none, top)
        part_out[1, frame] = part.astype(jnp.bfloat16)
        pl.when(has_after)(lambda: part_up(frame).start())
        pl.when(has_before)(lambda: part_down(frame).start())
        for r in range(rows):
            near = coarse[frame, r // 2]
            if r == 0:
                far = jnp.where(has_before, none, near)
            elif r == rows - 1:
                far = jnp.where(has_after, none, near)
            else:
                far = coarse[frame, r // 2 - 1] if r % 2 == 0 else coarse[frame, r // 2 + 1]
            second = conv_rows(f_ref, r - 1, 1 if r == 0 else 0, 2 if r == rows - 1 else 3, cols, w2_ref)
            joined = lifted(near, far) + moved[frame, r + HALO].astype(jnp.float32) + second
            if r == 0:
                edges[frame, 0] = joined
            elif r == rows - 1:
                edges[frame, 1] = joined
            else:
                mine[frame, r] = joined.astype(jnp.bfloat16)
        inner_copy(frame).start()
        return carry

    lax.fori_loop(0, own, conv_step, 0)

    def join_step(frame, carry):
        pl.when(has_before)(lambda: part_up(frame).wait_recv())
        mine[frame, 0] = (edges[frame, 0] + part_in[0, frame].astype(jnp.float32)).astype(jnp.bfloat16)
        edge_copy(frame, 0).start()
        pl.when(has_after)(lambda: part_down(frame).wait_recv())
        mine[frame, rows - 1] = (edges[frame, 1] + part_in[1, frame].astype(jnp.float32)).astype(jnp.bfloat16)
        edge_copy(frame, 1).start()
        return carry

    lax.fori_loop(0, own, join_step, 0)
    for frame in range(own):
        inner_copy(frame).wait()
        edge_copy(frame, 0).wait()
        edge_copy(frame, 1).wait()
        pl.when(has_after)(lambda: part_up(frame).wait_send())
        pl.when(has_before)(lambda: part_down(frame).wait_send())
    for shift in range(1, halves):
        for chunk in range(CHUNKS):
            fine_copy(shift, chunk).wait_send()
    both(pl.ds(0, own), pl.ds(0, span), 0, wait_send, wait_send)
    for chunk in range(1, CHUNKS):
        both(pl.ds(0, early), pl.ds(chunk * span, span), chunk, wait_send, wait_send)
    for frame in range(early, own):
        both(pl.ds(frame, 1), rest, CHUNKS + frame - early, wait_send, wait_send)


def local(fine, coarse, w_query, w_key, w_value, w_out, conv_first, conv_second):
    own, rows, cols, width = fine.shape
    _, half, small, _ = coarse.shape
    bands, halves = lax.axis_size("space"), lax.axis_size("tm")
    pieces = CHUNKS + own - own // 2
    far = own * (halves - 1)
    any_space = pl.BlockSpec(memory_space=pl.ANY)
    vmem = pl.BlockSpec(memory_space=pltpu.VMEM)
    bf16 = jnp.bfloat16
    return pl.pallas_call(
        functools.partial(kernel, bands, halves),
        in_specs=[any_space] * 2 + [vmem] * 5 + [any_space] * 2 + [vmem],
        out_specs=any_space,
        out_shape=jax.ShapeDtypeStruct(fine.shape, bf16),
        scratch_shapes=[
            pltpu.VMEM((own, rows, cols, width), bf16),
            pltpu.VMEM((far, rows, cols, width), bf16),
            pltpu.VMEM((own, rows + 2 * HALO, cols, width), bf16),
            pltpu.VMEM((own, half, small, width), bf16),
            pltpu.VMEM(((rows + 2 * HALO) * cols, 3 * width), bf16),
            pltpu.VMEM((rows * cols, 3 * width), bf16),
            pltpu.VMEM((9 * width, width), bf16),
            pltpu.VMEM((9 * width, width), bf16),
            pltpu.VMEM((own, 2, cols, width), jnp.float32),
            pltpu.VMEM((2, own, cols, width), bf16),
            pltpu.VMEM((2, own, cols, width), bf16),
            pltpu.SemaphoreType.DMA((CHUNKS + 3,)),
            pltpu.SemaphoreType.DMA((halves - 1, CHUNKS)),
            pltpu.SemaphoreType.DMA((halves - 1, CHUNKS)),
            pltpu.SemaphoreType.DMA((2, pieces)),
            pltpu.SemaphoreType.DMA((2, pieces)),
            pltpu.SemaphoreType.DMA((2, own)),
            pltpu.SemaphoreType.DMA((2, own)),
            pltpu.SemaphoreType.DMA((3, own)),
        ],
        compiler_params=pltpu.CompilerParams(
            collective_id=0, has_side_effects=True, vmem_limit_bytes=62 * 1024 * 1024
        ),
        name="fused",
    )(
        fine, coarse, jnp.asarray(encode(own * halves, width)), w_query, w_key, w_value, w_out,
        conv_first.reshape(9 * width, width), conv_second.reshape(9 * width, width), jnp.asarray(lift_matrix(small)),
    )


def solution(mesh):
    return jax.shard_map(
        local,
        mesh=mesh,
        in_specs=(
            P("tm", "space", None, None),
            P("tm", "space", None, None),
            P(),
            P(),
            P(),
            P(),
            P(),
            P(),
        ),
        out_specs=P("tm", "space", None, None),
        check_vma=False,
    )
```
